32 devices in a mesh: pq: 8 (over z, x), hh: 4 (over y, core).
Axes of the slice: x: 2, y: 2, z: 4, core: 2. Of those that a mesh axis runs over, the one named last changes fastest.
Arguments:
- amplitudes: bfloat16 [4096, 2048], P('hh', 'pq'), may hold values from -6 to 6
- integrals: bfloat16 [4096, 2048], P('hh', 'pq'), may hold values from -0.001953125 to 0.001953125
- left_amps: bfloat16 [8, 4096, 1024], P(None, 'hh', 'pq'), may hold values from -6 to 6
Outputs:
- sigma_ladder: bfloat16 [8, 4096, 1024], P(None, 'hh', 'pq')
- subspace: float32 [8, 8], replicated
The draws below stay inside these ranges and needn't reach their ends.
All inputs are finite; a program needn't handle non-finite values.
Results may differ from the reference program's by a relative error of at most 0.0049.
Values may be sent and summed in bfloat16 or wider, within the bound.
A program may use at most 64 MiB of HBM per device.

```python
import math
import jax
import jax.numpy as jnp
from jax import lax

OCC_PAIRS = 4096
ROOTS = 8
CD_PAIRS = 2048
AB_PAIRS = 1024


def levels(stream_key, extent, shards, smallest, largest):
    def one(dim, blocks):
        steps = jax.random.uniform(jax.random.fold_in(jax.random.fold_in(stream_key, 6), dim), (blocks,), jnp.float32, smallest / len(shards), largest / len(shards))
        return jnp.repeat(jnp.exp(steps), extent[dim] // blocks).reshape((-1,) + (1,) * (len(extent) - dim - 1))

    level = one(*shards[0])
    for cut in shards[1:]:
        level = level * one(*cut)
    return level


def centred(rng, shape, scale, bound, pieces=(), kind=jnp.bfloat16):
    entries = jax.random.normal(rng, shape, jnp.float32) * scale
    if len(pieces) > 0:
        entries = levels(rng, shape, pieces, -0.22, 0.18) * entries
    return jnp.clip(entries, min=-bound, max=bound).astype(kind)


def setup_inputs(seed: int = 0) -> dict:
    seeds = jax.random.split(jax.random.key(seed), 4)
    amplitudes = centred(seeds[0], (OCC_PAIRS, CD_PAIRS), 1.0, 6.0, ((0, 4), (1, 8)))
    integrals = centred(seeds[1], (OCC_PAIRS, CD_PAIRS), (CD_PAIRS * OCC_PAIRS) ** -0.5, 0.001953125, ((0, 4), (1, 8)))
    left_amps = centred(seeds[2], (ROOTS, OCC_PAIRS, AB_PAIRS), 1.0, 6.0, ((1, 4), (2, 8)))
    return dict(amplitudes=amplitudes, integrals=integrals, left_amps=left_amps)


def reference(amplitudes, integrals, left_amps):
    ladder = jnp.dot(amplitudes, integrals.T, preferred_element_type=jnp.float32).astype(jnp.bfloat16)
    ladder_trans = ladder.T

    def one_root(left_root):
        return jnp.dot(ladder_trans, left_root, preferred_element_type=jnp.float32).astype(jnp.bfloat16)
    sigma_ladder = lax.map(one_root, left_amps)
    flat_left = left_amps.reshape(ROOTS, -1)
    flat_sigma = sigma_ladder.reshape(ROOTS, -1)
    gram = jnp.dot(flat_left, flat_sigma.T, preferred_element_type=jnp.float32)
    subspace = gram * (1.0 / math.sqrt(OCC_PAIRS * AB_PAIRS))
    return (sigma_ladder, subspace)
```

```python
import functools
import math

import jax
import jax.numpy as jnp
from jax import lax
from jax.experimental import pallas as pl
from jax.experimental.pallas import tpu as pltpu
from jax.sharding import PartitionSpec as P

MESH = pl.DeviceIdType.MESH
SLOTS = 4
TILE = 256


def remote(src, dst, send_sem, recv_sem, where):
    return pltpu.make_async_remote_copy(
        src_ref=src,
        dst_ref=dst,
        send_sem=send_sem,
        recv_sem=recv_sem,
        device_id=where,
        device_id_type=MESH,
    )


def kernel(
    npq, nhh, factor,
    t_ref, i_ref, l_ref, out_ref, sub_ref,
    tbuf, ibuf, lbuf, pbuf, sibr, ysend, yrecv, mbuf, acc, sig, gram, red,
    load_sem, out_sem, fwd_sem, blk_sem, sib_ssem, sib_rsem,
    y_ssem, y_rsem, m_ssem, m_rsem, r_ssem, r_rsem,
):
    nx = nhh // 2
    nz, ny = npq // nx, nhh // 2
    roots, rows, ab = l_ref.shape
    depth = t_ref.shape[1]
    half = depth // 2
    me, hh = lax.axis_index("pq"), lax.axis_index("hh")
    z, x = me // nx, me % nx
    y, c = hh // 2, hh % 2
    sibling = {"hh": y * 2 + (1 - c)}
    mine = pl.ds(pl.multiple_of(c * half, half), half)
    other = pl.ds(pl.multiple_of((1 - c) * half, half), half)

    loads = [
        pltpu.make_async_copy(t_ref, tbuf.at[me], load_sem.at[0]),
        pltpu.make_async_copy(i_ref, ibuf.at[me], load_sem.at[1]),
    ] + [
        pltpu.make_async_copy(
            l_ref.at[r], lbuf.at[:, pl.ds(r * ab, ab)], load_sem.at[2 + r]
        )
        for r in range(roots)
    ]
    for load in loads:
        load.start()

    barrier = pltpu.get_barrier_semaphore()
    for d in range(1, npq):
        pl.semaphore_signal(
            barrier, inc=1, device_id={"pq": (me + d) % npq}, device_id_type=MESH
        )
    for d in range(1, nhh):
        pl.semaphore_signal(
            barrier, inc=1, device_id={"hh": (hh + d) % nhh}, device_id_type=MESH
        )
    pl.semaphore_wait(barrier, npq + nhh - 2)

    below, above = z, nz - 1 - z
    paired = jnp.minimum(below, above)

    def column(i):
        step = (i + 1) // 2 if i % 2 else -(i // 2)
        side = jnp.where(above > below, 1, -1)
        return z + jnp.where(i <= 2 * paired, step, side * (i - paired))

    def block_copy(kind, blk, way):
        buf = (tbuf, ibuf)[kind].at[blk]
        to = me + (nx, -nx, 1, -1)[way]
        return remote(
            buf, buf, fwd_sem.at[kind, blk, way], blk_sem.at[kind, blk], {"pq": to}
        )

    def ways(zz, xx):
        if xx is None:
            return [
                (2, x < nx - 1),
                (3, x > 0),
                (0, (zz <= z) & (z < nz - 1)),
                (1, (zz >= z) & (z > 0)),
            ]
        if nx == 2:
            return []
        return [(2, (xx < x) & (x < nx - 1)), (3, (xx > x) & (x > 0))]

    def place(zz, xx):
        return zz * nx + (x if xx is None else xx)

    def forward(kind, zz, xx):
        blk = place(zz, xx)
        for way, cond in ways(zz, xx):
            @pl.when(cond)
            def _():
                block_copy(kind, blk, way).start()

    def sent(kind, zz, xx):
        blk = place(zz, xx)
        for way, cond in ways(zz, xx):
            @pl.when(cond)
            def _():
                block_copy(kind, blk, way).wait_send()

    def arrived(kind, zz, xx):
        block_copy(kind, place(zz, xx), 0).wait_recv()

    zs = [column(i) for i in range(nz)]
    xs = [(x + j) % nx for j in range(1, nx)]

    loads[0].wait()
    forward(0, zs[0], None)
    loads[1].wait()
    forward(1, zs[0], None)
    for load in loads[2:]:
        load.wait()

    order = []

    def sib_copy(k):
        s = k % SLOTS
        return remote(
            pbuf.at[s, other], sibr.at[s], sib_ssem.at[s], sib_rsem.at[s], sibling
        )

    def y_copy(k, d):
        s = k % SLOTS
        return remote(
            ysend.at[s], yrecv.at[s, d - 1], y_ssem.at[s, d - 1], y_rsem.at[s, d - 1],
            {"hh": (y + d) % ny * 2 + c},
        )

    def m_copy(k):
        buf = mbuf.at[:, place(*order[k]), mine]
        return remote(buf, buf, m_ssem.at[k], m_rsem.at[k], sibling)

    def stage1(k):
        if k >= SLOTS:
            m_copy(k - SLOTS).wait_recv()
        s = k % SLOTS
        pbuf[s] = lax.dot_general(
            tbuf[place(*order[k])], lbuf[...], (((0,), (0,)), ((), ())),
            preferred_element_type=jnp.float32,
        )
        sib_copy(k).start()

    def stage2(k):
        s = k % SLOTS
        sib_copy(k).wait_recv()
        total = pbuf[s, mine] + sibr[s]
        pbuf[s, mine] = total
        if k >= SLOTS:
            for d in range(1, ny):
                y_copy(k - SLOTS, d).wait_send()
        ysend[s] = total.astype(jnp.bfloat16)
        for d in range(1, ny):
            y_copy(k, d).start()

    def stage3(k):
        s = k % SLOTS
        total = pbuf[s, mine]
        for d in range(1, ny):
            y_copy(k, d).wait_recv()
            total = total + yrecv[s, d - 1].astype(jnp.float32)
        high = total.astype(jnp.bfloat16)
        mbuf[0, place(*order[k]), mine] = high
        mbuf[1, place(*order[k]), mine] = (total - high.astype(jnp.float32)).astype(
            jnp.bfloat16
        )
        m_copy(k).start()
        sib_copy(k).wait_send()

    def t_event(zz, xx):
        k = len(order)
        order.append((zz, xx))
        if k > 0:
            arrived(0, zz, xx)
            forward(0, zz, xx)
        stage1(k)
        if k >= 1:
            stage2(k - 1)
        if k >= 2:
            stage3(k - 2)

    for i in range(nz + 1):
        if i < nz:
            t_event(zs[i], None)
        if i >= 1:
            for xx in xs:
                t_event(zs[i - 1], xx)
        if i >= 2:
            arrived(1, zs[i - 1], None)
            forward(1, zs[i - 1], None)
    count = len(order)
    stage2(count - 1)
    stage3(count - 2)
    stage3(count - 1)

    for k in range(count):
        zz, xx = order[k]
        if k > count - 1 - SLOTS:
            m_copy(k).wait_recv()
        if xx is not None:
            arrived(1, zz, xx)
            forward(1, zz, xx)
        blk = place(zz, xx)

        @pl.loop(0, rows // TILE)
        def _(j):
            at = pl.ds(pl.multiple_of(j * TILE, TILE), TILE)
            prod = jnp.dot(
                ibuf[blk, at], mbuf[0, blk], preferred_element_type=jnp.float32
            ) + jnp.dot(ibuf[blk, at], mbuf[1, blk], preferred_element_type=jnp.float32)
            if k > 0:
                prod = acc[at] + prod
            if k < count - 1:
                acc[at] = prod
            else:
                sig[at] = prod.astype(jnp.bfloat16)

    outs = [
        pltpu.make_async_copy(
            sig.at[:, pl.ds(r * ab, ab)], out_ref.at[r], out_sem.at[r]
        )
        for r in range(roots)
    ]
    for copy in outs:
        copy.start()

    lanes = lax.broadcasted_iota(jnp.int32, (ab, roots * ab), 1) % ab
    diag = lanes == lax.broadcasted_iota(jnp.int32, (ab, roots * ab), 0)

    @pl.loop(0, roots)
    def _(r):
        cols = pl.ds(pl.multiple_of(r * ab, ab), ab)
        g = lax.dot_general(
            lbuf[:, cols], sig[...], (((0,), (0,)), ((), ())),
            preferred_element_type=jnp.float32,
        )
        gram[pl.ds(r, 1)] = jnp.sum(jnp.where(diag, g, 0.0), axis=0, keepdims=True)

    lane = lax.broadcasted_iota(jnp.int32, (roots, 128), 1)
    local = jnp.zeros((roots, 128), jnp.float32)
    for s in range(roots):
        one = jnp.sum(gram[:, s * ab : (s + 1) * ab], axis=1, keepdims=True)
        local = jnp.where(lane == s, one, local)

    base = 0
    for axis, at, n in (("hh", hh, nhh), ("pq", me, npq)):
        red[base] = local
        copies = [
            remote(
                red.at[base], red.at[base + d], r_ssem.at[base + d],
                r_rsem.at[base + d], {axis: (at + d) % n},
            )
            for d in range(1, n)
        ]
        for copy in copies:
            copy.start()
        for copy in copies:
            copy.wait_recv()
        for d in range(1, n):
            local = local + red[base + d]
        for copy in copies:
            copy.wait_send()
        base += n
    sub_ref[...] = local[:, :roots] * factor

    for k in range(count):
        sent(0, *order[k])
        sent(1, *order[k])
        m_copy(k).wait_send()
    for k in range(max(0, count - SLOTS), count):
        for d in range(1, ny):
            y_copy(k, d).wait_send()
    for copy in outs:
        copy.wait()


def solution(mesh):
    npq, nhh = mesh.shape["pq"], mesh.shape["hh"]

    def body(amplitudes, integrals, left_amps):
        roots, rows, ab = left_amps.shape
        depth = amplitudes.shape[1]
        half, wide = depth // 2, roots * ab
        ny = nhh // 2
        factor = 1.0 / math.sqrt(rows * nhh * ab * npq)
        bf16, f32, dma = jnp.bfloat16, jnp.float32, pltpu.SemaphoreType.DMA
        return pl.pallas_call(
            functools.partial(kernel, npq, nhh, factor),
            out_shape=(
                jax.ShapeDtypeStruct(left_amps.shape, bf16),
                jax.ShapeDtypeStruct((roots, roots), f32),
            ),
            in_specs=[pl.BlockSpec(memory_space=pl.ANY)] * 3,
            out_specs=(
                pl.BlockSpec(memory_space=pl.ANY),
                pl.BlockSpec(memory_space=pltpu.VMEM),
            ),
            scratch_shapes=[
                pltpu.VMEM((npq, rows, depth), bf16),
                pltpu.VMEM((npq, rows, depth), bf16),
                pltpu.VMEM((rows, wide), bf16),
                pltpu.VMEM((SLOTS, depth, wide), f32),
                pltpu.VMEM((SLOTS, half, wide), f32),
                pltpu.VMEM((SLOTS, half, wide), bf16),
                pltpu.VMEM((SLOTS, ny - 1, half, wide), bf16),
                pltpu.VMEM((2, npq, depth, wide), bf16),
                pltpu.VMEM((rows, wide), f32),
                pltpu.VMEM((rows, wide), bf16),
                pltpu.VMEM((roots, wide), f32),
                pltpu.VMEM((nhh + npq, roots, 128), f32),
                dma((2 + roots,)),
                dma((roots,)),
                dma((2, npq, 4)),
                dma((2, npq)),
                dma((SLOTS,)),
                dma((SLOTS,)),
                dma((SLOTS, ny - 1)),
                dma((SLOTS, ny - 1)),
                dma((npq,)),
                dma((npq,)),
                dma((nhh + npq,)),
                dma((nhh + npq,)),
            ],
            compiler_params=pltpu.CompilerParams(
                collective_id=0,
                has_side_effects=True,
                vmem_limit_bytes=67043328,
            ),
        )(amplitudes, integrals, left_amps)

    return jax.shard_map(
        body,
        mesh=mesh,
        in_specs=(P("hh", "pq"), P("hh", "pq"), P(None, "hh", "pq")),
        out_specs=(P(None, "hh", "pq"), P()),
        check_vma=False,
    )
```

```python
import functools
import math

import jax
import jax.numpy as jnp
from jax import lax
from jax.experimental import pallas as pl
from jax.experimental.pallas import tpu as pltpu
from jax.sharding import PartitionSpec as P

MESH = pl.DeviceIdType.MESH
SLOTS = 4
TILE = 256


def remote(src, dst, send_sem, recv_sem, where):
    return pltpu.make_async_remote_copy(
        src_ref=src,
        dst_ref=dst,
        send_sem=send_sem,
        recv_sem=recv_sem,
        device_id=where,
        device_id_type=MESH,
    )


def kernel(
    npq, nhh, factor,
    t_ref, i_ref, l_ref, out_ref, sub_ref,
    tbuf, ibuf, lbuf, pbuf, sibr, ysend, yrecv, mbuf, acc, sig, gram, red,
    load_sem, out_sem, fwd_sem, blk_sem, sib_ssem, sib_rsem,
    y_ssem, y_rsem, m_ssem, m_rsem, r_ssem, r_rsem,
):
    nx = nhh // 2
    nz, ny = npq // nx, nhh // 2
    roots, rows, ab = l_ref.shape
    depth = t_ref.shape[1]
    half = depth // 2
    me, hh = lax.axis_index("pq"), lax.axis_index("hh")
    z, x = me // nx, me % nx
    y, c = hh // 2, hh % 2
    sibling = {"hh": y * 2 + (1 - c)}
    mine = pl.ds(pl.multiple_of(c * half, half), half)
    other = pl.ds(pl.multiple_of((1 - c) * half, half), half)

    loads = [
        pltpu.make_async_copy(t_ref, tbuf.at[me], load_sem.at[0]),
        pltpu.make_async_copy(i_ref, ibuf.at[me], load_sem.at[1]),
    ] + [
        pltpu.make_async_copy(
            l_ref.at[r], lbuf.at[:, pl.ds(r * ab, ab)], load_sem.at[2 + r]
        )
        for r in range(roots)
    ]
    for load in loads:
        load.start()

    barrier = pltpu.get_barrier_semaphore()
    for d in range(1, npq):
        pl.semaphore_signal(
            barrier, inc=1, device_id={"pq": (me + d) % npq}, device_id_type=MESH
        )
    for d in range(1, nhh):
        pl.semaphore_signal(
            barrier, inc=1, device_id={"hh": (hh + d) % nhh}, device_id_type=MESH
        )
    pl.semaphore_wait(barrier, npq + nhh - 2)

    below, above = z, nz - 1 - z
    paired = jnp.minimum(below, above)

    def column(i):
        step = (i + 1) // 2 if i % 2 else -(i // 2)
        side = jnp.where(above > below, 1, -1)
        return z + jnp.where(i <= 2 * paired, step, side * (i - paired))

    def block_copy(kind, blk, way):
        buf = (tbuf, ibuf)[kind].at[blk]
        to = me + (nx, -nx, 1, -1)[way]
        return remote(
            buf, buf, fwd_sem.at[kind, blk, way], blk_sem.at[kind, blk], {"pq": to}
        )

    balanced = nx == 2 and nz % 2 == 0
    partner = z + 1 - 2 * (z % 2)

    def ways(kind, zz, xx):
        if xx is None:
            cross = (zz != partner) if balanced and kind == 1 else (zz >= 0)
            return [
                (2, (x < nx - 1) & cross),
                (3, (x > 0) & cross),
                (0, (zz <= z) & (z < nz - 1)),
                (1, (zz >= z) & (z > 0)),
            ]
        if balanced and kind == 1:
            return [(0, (zz == z) & (partner > z)), (1, (zz == z) & (partner < z))]
        if nx == 2:
            return []
        return [(2, (xx < x) & (x < nx - 1)), (3, (xx > x) & (x > 0))]

    def place(zz, xx):
        return zz * nx + (x if xx is None else xx)

    def forward(kind, zz, xx):
        blk = place(zz, xx)
        for way, cond in ways(kind, zz, xx):
            @pl.when(cond)
            def _():
                block_copy(kind, blk, way).start()

    def sent(kind, zz, xx):
        blk = place(zz, xx)
        for way, cond in ways(kind, zz, xx):
            @pl.when(cond)
            def _():
                block_copy(kind, blk, way).wait_send()

    def arrived(kind, zz, xx):
        block_copy(kind, place(zz, xx), 0).wait_recv()

    zs = [column(i) for i in range(nz)]
    xs = [(x + j) % nx for j in range(1, nx)]

    loads[0].wait()
    forward(0, zs[0], None)
    loads[1].wait()
    forward(1, zs[0], None)
    for load in loads[2:]:
        load.wait()

    order = []

    def sib_copy(k):
        s = k % SLOTS
        return remote(
            pbuf.at[s, other], sibr.at[s], sib_ssem.at[s], sib_rsem.at[s], sibling
        )

    def y_copy(k, d):
        s = k % SLOTS
        return remote(
            ysend.at[s], yrecv.at[s, d - 1], y_ssem.at[s, d - 1], y_rsem.at[s, d - 1],
            {"hh": (y + d) % ny * 2 + c},
        )

    def m_copy(k):
        buf = mbuf.at[:, place(*order[k]), mine]
        return remote(buf, buf, m_ssem.at[k], m_rsem.at[k], sibling)

    def stage1(k):
        if k >= SLOTS:
            m_copy(k - SLOTS).wait_recv()
        s = k % SLOTS
        pbuf[s] = lax.dot_general(
            tbuf[place(*order[k])], lbuf[...], (((0,), (0,)), ((), ())),
            preferred_element_type=jnp.float32,
        )
        sib_copy(k).start()

    def stage2(k):
        s = k % SLOTS
        sib_copy(k).wait_recv()
        total = pbuf[s, mine] + sibr[s]
        pbuf[s, mine] = total
        if k >= SLOTS:
            for d in range(1, ny):
                y_copy(k - SLOTS, d).wait_send()
        ysend[s] = total.astype(jnp.bfloat16)
        for d in range(1, ny):
            y_copy(k, d).start()

    def stage3(k):
        s = k % SLOTS
        total = pbuf[s, mine]
        for d in range(1, ny):
            y_copy(k, d).wait_recv()
            total = total + yrecv[s, d - 1].astype(jnp.float32)
        high = total.astype(jnp.bfloat16)
        mbuf[0, place(*order[k]), mine] = high
        mbuf[1, place(*order[k]), mine] = (total - high.astype(jnp.float32)).astype(
            jnp.bfloat16
        )
        m_copy(k).start()
        sib_copy(k).wait_send()

    def t_event(zz, xx):
        k = len(order)
        order.append((zz, xx))
        if k > 0:
            arrived(0, zz, xx)
            forward(0, zz, xx)
        stage1(k)
        if k >= 1:
            stage2(k - 1)
        if k >= 2:
            stage3(k - 2)

    for i in range(nz + 1):
        if i < nz:
            t_event(zs[i], None)
        if i >= 1:
            for xx in xs:
                t_event(zs[i - 1], xx)
        if i >= 2:
            arrived(1, zs[i - 1], None)
            forward(1, zs[i - 1], None)
        if i == 2 and balanced:
            arrived(1, zs[0], xs[0])
            forward(1, zs[0], xs[0])
    count = len(order)
    stage2(count - 1)
    stage3(count - 2)
    stage3(count - 1)

    first_cross = min(k for k in range(count) if order[k][1] is not None)
    for k in range(count):
        zz, xx = order[k]
        if k > count - 1 - SLOTS:
            m_copy(k).wait_recv()
        if xx is not None and not (balanced and k == first_cross):
            arrived(1, zz, xx)
            forward(1, zz, xx)
        blk = place(zz, xx)

        @pl.loop(0, rows // TILE)
        def _(j):
            at = pl.ds(pl.multiple_of(j * TILE, TILE), TILE)
            prod = jnp.dot(
                ibuf[blk, at], mbuf[0, blk], preferred_element_type=jnp.float32
            ) + jnp.dot(ibuf[blk, at], mbuf[1, blk], preferred_element_type=jnp.float32)
            if k > 0:
                prod = acc[at] + prod
            if k < count - 1:
                acc[at] = prod
            else:
                sig[at] = prod.astype(jnp.bfloat16)

    outs = [
        pltpu.make_async_copy(
            sig.at[:, pl.ds(r * ab, ab)], out_ref.at[r], out_sem.at[r]
        )
        for r in range(roots)
    ]
    for copy in outs:
        copy.start()

    lanes = lax.broadcasted_iota(jnp.int32, (ab, roots * ab), 1) % ab
    diag = lanes == lax.broadcasted_iota(jnp.int32, (ab, roots * ab), 0)

    @pl.loop(0, roots)
    def _(r):
        cols = pl.ds(pl.multiple_of(r * ab, ab), ab)
        g = lax.dot_general(
            lbuf[:, cols], sig[...], (((0,), (0,)), ((), ())),
            preferred_element_type=jnp.float32,
        )
        gram[pl.ds(r, 1)] = jnp.sum(jnp.where(diag, g, 0.0), axis=0, keepdims=True)

    lane = lax.broadcasted_iota(jnp.int32, (roots, 128), 1)
    local = jnp.zeros((roots, 128), jnp.float32)
    for s in range(roots):
        one = jnp.sum(gram[:, s * ab : (s + 1) * ab], axis=1, keepdims=True)
        local = jnp.where(lane == s, one, local)

    base = 0
    for axis, at, n in (("hh", hh, nhh), ("pq", me, npq)):
        red[base] = local
        copies = [
            remote(
                red.at[base], red.at[base + d], r_ssem.at[base + d],
                r_rsem.at[base + d], {axis: (at + d) % n},
            )
            for d in range(1, n)
        ]
        for copy in copies:
            copy.start()
        for copy in copies:
            copy.wait_recv()
        for d in range(1, n):
            local = local + red[base + d]
        for copy in copies:
            copy.wait_send()
        base += n
    sub_ref[...] = local[:, :roots] * factor

    for k in range(count):
        sent(0, *order[k])
        sent(1, *order[k])
        m_copy(k).wait_send()
    for k in range(max(0, count - SLOTS), count):
        for d in range(1, ny):
            y_copy(k, d).wait_send()
    for copy in outs:
        copy.wait()


def solution(mesh):
    npq, nhh = mesh.shape["pq"], mesh.shape["hh"]

    def body(amplitudes, integrals, left_amps):
        roots, rows, ab = left_amps.shape
        depth = amplitudes.shape[1]
        half, wide = depth // 2, roots * ab
        ny = nhh // 2
        factor = 1.0 / math.sqrt(rows * nhh * ab * npq)
        bf16, f32, dma = jnp.bfloat16, jnp.float32, pltpu.SemaphoreType.DMA
        return pl.pallas_call(
            functools.partial(kernel, npq, nhh, factor),
            out_shape=(
                jax.ShapeDtypeStruct(left_amps.shape, bf16),
                jax.ShapeDtypeStruct((roots, roots), f32),
            ),
            in_specs=[pl.BlockSpec(memory_space=pl.ANY)] * 3,
            out_specs=(
                pl.BlockSpec(memory_space=pl.ANY),
                pl.BlockSpec(memory_space=pltpu.VMEM),
            ),
            scratch_shapes=[
                pltpu.VMEM((npq, rows, depth), bf16),
                pltpu.VMEM((npq, rows, depth), bf16),
                pltpu.VMEM((rows, wide), bf16),
                pltpu.VMEM((SLOTS, depth, wide), f32),
                pltpu.VMEM((SLOTS, half, wide), f32),
                pltpu.VMEM((SLOTS, half, wide), bf16),
                pltpu.VMEM((SLOTS, ny - 1, half, wide), bf16),
                pltpu.VMEM((2, npq, depth, wide), bf16),
                pltpu.VMEM((rows, wide), f32),
                pltpu.VMEM((rows, wide), bf16),
                pltpu.VMEM((roots, wide), f32),
                pltpu.VMEM((nhh + npq, roots, 128), f32),
                dma((2 + roots,)),
                dma((roots,)),
                dma((2, npq, 4)),
                dma((2, npq)),
                dma((SLOTS,)),
                dma((SLOTS,)),
                dma((SLOTS, ny - 1)),
                dma((SLOTS, ny - 1)),
                dma((npq,)),
                dma((npq,)),
                dma((nhh + npq,)),
                dma((nhh + npq,)),
            ],
            compiler_params=pltpu.CompilerParams(
                collective_id=0,
                has_side_effects=True,
                vmem_limit_bytes=67043328,
            ),
        )(amplitudes, integrals, left_amps)

    return jax.shard_map(
        body,
        mesh=mesh,
        in_specs=(P("hh", "pq"), P("hh", "pq"), P(None, "hh", "pq")),
        out_specs=(P(None, "hh", "pq"), P()),
        check_vma=False,
    )
```

```python
import functools
import math

import jax
import jax.numpy as jnp
from jax import lax
from jax.experimental import pallas as pl
from jax.experimental.pallas import tpu as pltpu
from jax.sharding import PartitionSpec as P

MESH = pl.DeviceIdType.MESH
SLOTS = 4
TILE = 256


def remote(src, dst, send_sem, recv_sem, where):
    return pltpu.make_async_remote_copy(
        src_ref=src,
        dst_ref=dst,
        send_sem=send_sem,
        recv_sem=recv_sem,
        device_id=where,
        device_id_type=MESH,
    )


def kernel(
    npq, nhh, factor,
    t_ref, i_ref, l_ref, out_ref, sub_ref,
    tbuf, ibuf, lbuf, pbuf, sibr, ysend, yrecv, mbuf, acc, sig, gram, red,
    load_sem, out_sem, fwd_sem, blk_sem, sib_ssem, sib_rsem,
    y_ssem, y_rsem, m_ssem, m_rsem, r_ssem, r_rsem,
):
    nx = nhh // 2
    nz, ny = npq // nx, nhh // 2
    roots, rows, ab = l_ref.shape
    depth = t_ref.shape[1]
    half = depth // 2
    me, hh = lax.axis_index("pq"), lax.axis_index("hh")
    z, x = me // nx, me % nx
    y, c = hh // 2, hh % 2
    sibling = {"hh": y * 2 + (1 - c)}
    mine = pl.ds(pl.multiple_of(c * half, half), half)
    other = pl.ds(pl.multiple_of((1 - c) * half, half), half)

    loads = [
        pltpu.make_async_copy(t_ref, tbuf.at[me], load_sem.at[0]),
        pltpu.make_async_copy(i_ref, ibuf.at[me], load_sem.at[1]),
    ] + [
        pltpu.make_async_copy(
            l_ref.at[r], lbuf.at[:, pl.ds(r * ab, ab)], load_sem.at[2 + r]
        )
        for r in range(roots)
    ]
    for load in loads:
        load.start()

    barrier = pltpu.get_barrier_semaphore()
    for d in range(1, npq):
        pl.semaphore_signal(
            barrier, inc=1, device_id={"pq": (me + d) % npq}, device_id_type=MESH
        )
    for d in range(1, nhh):
        pl.semaphore_signal(
            barrier, inc=1, device_id={"hh": (hh + d) % nhh}, device_id_type=MESH
        )
    pl.semaphore_wait(barrier, npq + nhh - 2)

    below, above = z, nz - 1 - z
    paired = jnp.minimum(below, above)

    def column(i):
        step = (i + 1) // 2 if i % 2 else -(i // 2)
        side = jnp.where(above > below, 1, -1)
        return z + jnp.where(i <= 2 * paired, step, side * (i - paired))

    def block_copy(kind, blk, way):
        buf = (tbuf, ibuf)[kind].at[blk]
        to = me + (nx, -nx, 1, -1)[way]
        return remote(
            buf, buf, fwd_sem.at[kind, blk, way], blk_sem.at[kind, blk], {"pq": to}
        )

    def ways(zz, xx):
        if xx is None:
            return [
                (2, x < nx - 1),
                (3, x > 0),
                (0, (zz <= z) & (z < nz - 1)),
                (1, (zz >= z) & (z > 0)),
            ]
        if nx == 2:
            return []
        return [(2, (xx < x) & (x < nx - 1)), (3, (xx > x) & (x > 0))]

    def place(zz, xx):
        return zz * nx + (x if xx is None else xx)

    def forward(kind, zz, xx):
        blk = place(zz, xx)
        for way, cond in ways(zz, xx):
            @pl.when(cond)
            def _():
                block_copy(kind, blk, way).start()

    def sent(kind, zz, xx):
        blk = place(zz, xx)
        for way, cond in ways(zz, xx):
            @pl.when(cond)
            def _():
                block_copy(kind, blk, way).wait_send()

    def arrived(kind, zz, xx):
        block_copy(kind, place(zz, xx), 0).wait_recv()

    zs = [column(i) for i in range(nz)]
    xs = [(x + j) % nx for j in range(1, nx)]

    loads[0].wait()
    forward(0, zs[0], None)
    loads[1].wait()
    forward(1, zs[0], None)
    for load in loads[2:]:
        load.wait()

    order = []

    def sib_copy(k):
        s = k % SLOTS
        return remote(
            pbuf.at[s, other], sibr.at[s], sib_ssem.at[s], sib_rsem.at[s], sibling
        )

    def y_copy(k, d):
        s = k % SLOTS
        return remote(
            ysend.at[s], yrecv.at[s, d - 1], y_ssem.at[s, d - 1], y_rsem.at[s, d - 1],
            {"hh": (y + d) % ny * 2 + c},
        )

    def m_copy(k):
        buf = mbuf.at[:, place(*order[k]), mine]
        return remote(buf, buf, m_ssem.at[k], m_rsem.at[k], sibling)

    def stage1(k):
        if k >= SLOTS:
            m_copy(k - SLOTS).wait_recv()
        s = k % SLOTS
        pbuf[s] = lax.dot_general(
            tbuf[place(*order[k])], lbuf[...], (((0,), (0,)), ((), ())),
            preferred_element_type=jnp.float32,
        )
        sib_copy(k).start()

    def stage2(k):
        s = k % SLOTS
        sib_copy(k).wait_recv()
        total = pbuf[s, mine] + sibr[s]
        pbuf[s, mine] = total
        if k >= SLOTS:
            for d in range(1, ny):
                y_copy(k - SLOTS, d).wait_send()
        ysend[s] = total.astype(jnp.bfloat16)
        for d in range(1, ny):
            y_copy(k, d).start()

    def stage3(k):
        s = k % SLOTS
        total = pbuf[s, mine]
        for d in range(1, ny):
            y_copy(k, d).wait_recv()
            total = total + yrecv[s, d - 1].astype(jnp.float32)
        high = total.astype(jnp.bfloat16)
        mbuf[0, place(*order[k]), mine] = high
        mbuf[1, place(*order[k]), mine] = (total - high.astype(jnp.float32)).astype(
            jnp.bfloat16
        )
        m_copy(k).start()
        sib_copy(k).wait_send()

    def t_event(zz, xx):
        k = len(order)
        order.append((zz, xx))
        if k > 0:
            arrived(0, zz, xx)
            forward(0, zz, xx)
        stage1(k)
        if k >= 1:
            stage2(k - 1)
        if k >= 2:
            stage3(k - 2)

    for i in range(nz + 1):
        ahead = []
        if i < nz:
            t_event(zs[i], None)
        if i == nz - 1:
            ahead = range(1, nz - 2)
        if i == nz:
            ahead = range(max(1, nz - 2), nz)
        for j in ahead:
            arrived(1, zs[j], None)
            forward(1, zs[j], None)
        if i >= 1:
            for xx in xs:
                t_event(zs[i - 1], xx)
    count = len(order)
    stage2(count - 1)
    stage3(count - 2)
    stage3(count - 1)

    for k in range(count):
        zz, xx = order[k]
        if k > count - 1 - SLOTS:
            m_copy(k).wait_recv()
        if xx is not None:
            arrived(1, zz, xx)
            forward(1, zz, xx)
        blk = place(zz, xx)

        @pl.loop(0, rows // TILE)
        def _(j):
            at = pl.ds(pl.multiple_of(j * TILE, TILE), TILE)
            prod = jnp.dot(
                ibuf[blk, at], mbuf[0, blk], preferred_element_type=jnp.float32
            ) + jnp.dot(ibuf[blk, at], mbuf[1, blk], preferred_element_type=jnp.float32)
            if k > 0:
                prod = acc[at] + prod
            if k < count - 1:
                acc[at] = prod
            else:
                sig[at] = prod.astype(jnp.bfloat16)

    outs = [
        pltpu.make_async_copy(
            sig.at[:, pl.ds(r * ab, ab)], out_ref.at[r], out_sem.at[r]
        )
        for r in range(roots)
    ]
    for copy in outs:
        copy.start()

    lanes = lax.broadcasted_iota(jnp.int32, (ab, roots * ab), 1) % ab
    diag = lanes == lax.broadcasted_iota(jnp.int32, (ab, roots * ab), 0)

    @pl.loop(0, roots)
    def _(r):
        cols = pl.ds(pl.multiple_of(r * ab, ab), ab)
        g = lax.dot_general(
            lbuf[:, cols], sig[...], (((0,), (0,)), ((), ())),
            preferred_element_type=jnp.float32,
        )
        gram[pl.ds(r, 1)] = jnp.sum(jnp.where(diag, g, 0.0), axis=0, keepdims=True)

    lane = lax.broadcasted_iota(jnp.int32, (roots, 128), 1)
    local = jnp.zeros((roots, 128), jnp.float32)
    for s in range(roots):
        one = jnp.sum(gram[:, s * ab : (s + 1) * ab], axis=1, keepdims=True)
        local = jnp.where(lane == s, one, local)

    base = 0
    for axis, at, n in (("hh", hh, nhh), ("pq", me, npq)):
        red[base] = local
        copies = [
            remote(
                red.at[base], red.at[base + d], r_ssem.at[base + d],
                r_rsem.at[base + d], {axis: (at + d) % n},
            )
            for d in range(1, n)
        ]
        for copy in copies:
            copy.start()
        for copy in copies:
            copy.wait_recv()
        for d in range(1, n):
            local = local + red[base + d]
        for copy in copies:
            copy.wait_send()
        base += n
    sub_ref[...] = local[:, :roots] * factor

    for k in range(count):
        sent(0, *order[k])
        sent(1, *order[k])
        m_copy(k).wait_send()
    for k in range(max(0, count - SLOTS), count):
        for d in range(1, ny):
            y_copy(k, d).wait_send()
    for copy in outs:
        copy.wait()


def solution(mesh):
    npq, nhh = mesh.shape["pq"], mesh.shape["hh"]

    def body(amplitudes, integrals, left_amps):
        roots, rows, ab = left_amps.shape
        depth = amplitudes.shape[1]
        half, wide = depth // 2, roots * ab
        ny = nhh // 2
        factor = 1.0 / math.sqrt(rows * nhh * ab * npq)
        bf16, f32, dma = jnp.bfloat16, jnp.float32, pltpu.SemaphoreType.DMA
        return pl.pallas_call(
            functools.partial(kernel, npq, nhh, factor),
            out_shape=(
                jax.ShapeDtypeStruct(left_amps.shape, bf16),
                jax.ShapeDtypeStruct((roots, roots), f32),
            ),
            in_specs=[pl.BlockSpec(memory_space=pl.ANY)] * 3,
            out_specs=(
                pl.BlockSpec(memory_space=pl.ANY),
                pl.BlockSpec(memory_space=pltpu.VMEM),
            ),
            scratch_shapes=[
                pltpu.VMEM((npq, rows, depth), bf16),
                pltpu.VMEM((npq, rows, depth), bf16),
                pltpu.VMEM((rows, wide), bf16),
                pltpu.VMEM((SLOTS, depth, wide), f32),
                pltpu.VMEM((SLOTS, half, wide), f32),
                pltpu.VMEM((SLOTS, half, wide), bf16),
                pltpu.VMEM((SLOTS, ny - 1, half, wide), bf16),
                pltpu.VMEM((2, npq, depth, wide), bf16),
                pltpu.VMEM((rows, wide), f32),
                pltpu.VMEM((rows, wide), bf16),
                pltpu.VMEM((roots, wide), f32),
                pltpu.VMEM((nhh + npq, roots, 128), f32),
                dma((2 + roots,)),
                dma((roots,)),
                dma((2, npq, 4)),
                dma((2, npq)),
                dma((SLOTS,)),
                dma((SLOTS,)),
                dma((SLOTS, ny - 1)),
                dma((SLOTS, ny - 1)),
                dma((npq,)),
                dma((npq,)),
                dma((nhh + npq,)),
                dma((nhh + npq,)),
            ],
            compiler_params=pltpu.CompilerParams(
                collective_id=0,
                has_side_effects=True,
                vmem_limit_bytes=67043328,
            ),
        )(amplitudes, integrals, left_amps)

    return jax.shard_map(
        body,
        mesh=mesh,
        in_specs=(P("hh", "pq"), P("hh", "pq"), P(None, "hh", "pq")),
        out_specs=(P(None, "hh", "pq"), P()),
        check_vma=False,
    )
```
